32 devices in a mesh: dp: 16 (over z, y, core), mp: 2 (over x).
Axes of the slice: x: 2, y: 2, z: 4, core: 2. Of those that a mesh axis runs over, the one named last changes fastest.
Arguments:
- inputs: bfloat16 [4, 4096, 4096], P(None, 'dp'), may hold values from -60 to 60
- gate_cotangent: bfloat16 [4, 4096, 6144], P(None, 'dp', 'mp'), may hold values from -6 to 6
- ff_blocks: int32 [4], replicated, may hold values from 24 to 48, as said below
- layer_active: int32 [4], replicated, may hold values from 0 to 1, as said below
- param: float32 [4096, 6144], P(('dp', 'mp')), may hold values from -0.09375 to 0.09375
- moment: float32 [4096, 6144], P(('dp', 'mp')), may hold values from -3 to 3
- second_moment: float32 [4096, 6144], P(('dp', 'mp')), may hold values from 0.5 to 2
Outputs:
- new_param: float32 [4096, 6144], P(('dp', 'mp'))
- new_moment: float32 [4096, 6144], P(('dp', 'mp'))
- new_second: float32 [4096, 6144], P(('dp', 'mp'))
The draws below stay inside these ranges and needn't reach their ends.
Inputs may be any that keep to these rules, and one draw needn't show every extreme that they name: `ff_blocks`: entry 0 is 6144 // 128 (the largest subnet), entry 1 is 6144 // (256) (the smallest). `layer_active`: entry 0 is 1, and exactly one of entries 1, 2 and 3 is 0.
All inputs are finite; a program needn't handle non-finite values.
Results may differ from the reference program's by a relative error of at most 0.0003.
Values sent between devices are 32-bit elements; how exact they have to be, the bound alone decides.
A program may use at most 128 MiB of HBM per device.

```python
import math
import jax
import jax.numpy as jnp
from jax import lax

D = 4096
FF = 6144
BLOCK = 128
SUBNETS = 4
STEP = 10
TOK_DEV = 256
TOKENS = 4096


def draw_inputs(key, part):
    base = jnp.clip(jax.random.normal(jax.random.fold_in(key, 5), (SUBNETS, TOKENS, D), jnp.float32), -4.0, 4.0)
    column = lax.broadcasted_iota(jnp.int32, (D,), 0)
    place = column.astype(jnp.float32) / D
    scale = 1.0 + 2.0 * place
    replicas = TOKENS // TOK_DEV
    order = jax.random.permutation(jax.random.fold_in(key, 7), replicas).astype(jnp.int32)
    owner = lax.broadcasted_iota(jnp.int32, (TOKENS,), 0) // TOK_DEV
    paired = order[owner]
    column_block = column // (D // replicas)
    boost = jnp.where(column_block[None, :] == paired[:, None], 3.0, 1.0)
    return (base * scale[None, None, :] * boost[None, :, :]).astype(jnp.bfloat16)


def draw_ff_blocks(key, part):
    most = FF // BLOCK
    half = most // 2
    first = jax.random.randint(jax.random.fold_in(key, 11), (1,), half, most + 1)
    second = jax.random.randint(jax.random.fold_in(key, 13), (1,), half, most + 1)
    head = jnp.array([most, half], jnp.int32)
    return jnp.concatenate([head, first.astype(jnp.int32), second.astype(jnp.int32), jnp.full((SUBNETS - 4,), most, jnp.int32)]).astype(jnp.int32)


def draw_layer_active(key, part):
    pick = jax.random.randint(jax.random.fold_in(key, 23), (), 1, 4)
    index = lax.broadcasted_iota(jnp.int32, (SUBNETS,), 0)
    return jnp.where(index == pick, 0, 1).astype(jnp.int32)


def block_scale(stream_key, dims, shards, smallest, high):
    gain, own = 1.0, jax.random.fold_in(stream_key, 6)
    for dim, parts in shards:
        draws = jnp.exp(jax.random.uniform(jax.random.fold_in(own, dim), (parts,), jnp.float32, smallest / len(shards), high / len(shards)))
        gain = gain * jnp.repeat(draws, dims[dim] // parts).reshape([-1 if axis == dim else 1 for axis in range(len(dims))])
    return gain


def normal_values(rng, shape, width, limit, shards=(), held_as=jnp.bfloat16):
    values = width * jax.random.normal(rng, shape, jnp.float32)
    if shards:
        values = values * block_scale(rng, shape, shards, -0.22, 0.18)
    return jnp.clip(values, -limit, limit).astype(held_as)


def setup_inputs(seed: int = 0) -> dict:
    key_list = jax.random.split(jax.random.key(seed), 8)
    return {
        "inputs": draw_inputs(jax.random.fold_in(key_list[7], 71), 0),
        "gate_cotangent": normal_values(key_list[1], (SUBNETS, TOKENS, FF), 1.0, 6.0, ((1, 16), (2, 2))),
        "ff_blocks": draw_ff_blocks(jax.random.fold_in(key_list[7], 71), 0),
        "layer_active": draw_layer_active(jax.random.fold_in(key_list[7], 71), 0),
        "param": normal_values(key_list[4], (D, FF), D ** -0.5, 0.09375, ((0, 32),), jnp.float32),
        "moment": normal_values(key_list[5], (D, FF), 0.5, 3.0, ((0, 32),), jnp.float32),
        "second_moment": jnp.clip(jnp.exp(math.log(2.0) - 1.3862944 * jax.random.uniform(key_list[6], (D, FF), jnp.float32) ** block_scale(key_list[6], (D, FF), ((0, 32),), -0.2, 0.2)), 0.5, 2.0),
    }


def reference(inputs, gate_cotangent, ff_blocks, layer_active, param, moment, second_moment):
    column = lax.broadcasted_iota(jnp.int32, (SUBNETS, FF), 1)
    keep = (column < BLOCK * ff_blocks[:, None]) & (layer_active[:, None] == 1)
    masked = jnp.where(keep[:, None, :], gate_cotangent, jnp.zeros((), jnp.bfloat16))
    rows_in = inputs.reshape(SUBNETS * TOKENS, D)
    rows_ct = masked.reshape(SUBNETS * TOKENS, FF)
    gradient = lax.dot_general(rows_in, rows_ct, (((0,), (0,)), ((), ())), preferred_element_type=jnp.float32)
    total = jnp.sqrt(jnp.sum(gradient * gradient))
    factor = jnp.minimum(1.0, jnp.sqrt(1.0 * D * FF) / (total + 1e-06))
    clipped = gradient * factor
    new_moment = 0.9 * moment + 0.1 * clipped
    new_second = 0.95 * second_moment + 0.05 * clipped * clipped
    first_hat = new_moment / (1.0 - 0.9 ** STEP)
    second_hat = new_second / (1.0 - 0.95 ** STEP)
    new_param = param - 0.02 * (first_hat / (jnp.sqrt(second_hat) + 1e-08) + 0.1 * param)
    return (new_param, new_moment, new_second)
```

```python
import math

import jax
import jax.numpy as jnp
from jax import lax
from jax.sharding import PartitionSpec as P

D = 4096
FF = 6144
BLOCK = 128
STEP = 10


CHUNKS = 4


def exchange(values, bit, replicas):
    return lax.ppermute(values, "dp", [(i, i ^ (1 << bit)) for i in range(replicas)])


def product(rows_in, rows_ct):
    return lax.dot_general(
        rows_in, rows_ct, (((0,), (0,)), ((), ())), preferred_element_type=jnp.float32
    )


def halving_sum(rows_in, rows_ct, second_bit_first):
    replicas = lax.axis_size("dp")
    bits = replicas.bit_length() - 1
    me = lax.axis_index("dp")
    rows, width = rows_in.shape
    each = width // replicas
    blocks = rows_in.reshape(rows, replicas // 2, 2, each)

    def columns_of(bit):
        return lax.dynamic_index_in_dim(blocks, bit, 2, keepdims=False).reshape(rows, width // 2)

    mine = me % 2
    other = product(columns_of(1 - mine), rows_ct)
    held = product(columns_of(mine), rows_ct) + exchange(other, 0, replicas)
    left = list(range(bits - 1, 0, -1))
    cols = held.shape[1]
    held = held.reshape((2,) * len(left) + (each, cols))
    order = list(range(1, bits))
    if second_bit_first:
        order[:2] = order[:2][::-1]
    for bit in order:
        axis = left.index(bit)
        mine = (me // (1 << bit)) % 2
        sent = lax.dynamic_index_in_dim(held, 1 - mine, axis, keepdims=False)
        kept = lax.dynamic_index_in_dim(held, mine, axis, keepdims=False)
        held = kept + exchange(sent, bit, replicas)
        left.remove(bit)
    return held.reshape(each, cols)


def squared_total(values):
    return lax.psum(jnp.sum(values * values), ("dp", "mp"))


def shards(inputs, gate_cotangent, ff_blocks, layer_active, param, moment, second_moment):
    subnets, tokens, width = inputs.shape
    local_cols = gate_cotangent.shape[2]
    first_col = lax.axis_index("mp") * local_cols
    column = first_col + lax.broadcasted_iota(jnp.int32, (subnets, local_cols), 1)
    keep = (column < BLOCK * ff_blocks[:, None]) & (layer_active[:, None] == 1)
    masked = jnp.where(keep[:, None, :], gate_cotangent, jnp.zeros((), jnp.bfloat16))
    rows_in = inputs.reshape(subnets * tokens, width)
    rows_ct = masked.reshape(subnets * tokens, local_cols)
    tile = jnp.concatenate(
        [
            halving_sum(rows_in, part, second_bit_first=(place == CHUNKS - 1))
            for place, part in enumerate(jnp.split(rows_ct, CHUNKS, axis=1))
        ],
        axis=1,
    )
    owners = lax.axis_size("mp")
    pieces = lax.all_to_all(
        tile.reshape(owners, tile.shape[0] // owners, local_cols), "mp", split_axis=0, concat_axis=0
    )
    gradient = jnp.concatenate([pieces[i] for i in range(owners)], axis=1)
    total_sq = squared_total(gradient)
    total = jnp.sqrt(total_sq)
    factor = jnp.minimum(1.0, math.sqrt(1.0 * D * FF) / (total + 1e-06))
    clipped = gradient * factor
    new_moment = 0.9 * moment + 0.1 * clipped
    new_second = 0.95 * second_moment + 0.05 * clipped * clipped
    first_hat = new_moment / (1.0 - 0.9**STEP)
    second_hat = new_second / (1.0 - 0.95**STEP)
    new_param = param - 0.02 * (first_hat / (jnp.sqrt(second_hat) + 1e-08) + 0.1 * param)
    return (new_param, new_moment, new_second)


def solution(mesh):
    in_specs = (
        P(None, "dp", None),
        P(None, "dp", "mp"),
        P(),
        P(),
        P(("dp", "mp"), None),
        P(("dp", "mp"), None),
        P(("dp", "mp"), None),
    )
    out_specs = (P(("dp", "mp"), None), P(("dp", "mp"), None), P(("dp", "mp"), None))
    return jax.shard_map(shards, mesh=mesh, in_specs=in_specs, out_specs=out_specs, check_vma=False)
```

```python
import math

import jax
import jax.numpy as jnp
from jax import lax
from jax.sharding import PartitionSpec as P

D = 4096
FF = 6144
BLOCK = 128
STEP = 10


CHUNKS = 4


def exchange(values, bit, replicas):
    return lax.ppermute(values, "dp", [(i, i ^ (1 << bit)) for i in range(replicas)])


def product(rows_in, rows_ct):
    return lax.dot_general(
        rows_in, rows_ct, (((0,), (0,)), ((), ())), preferred_element_type=jnp.float32
    )


def halving_sum(rows_in, rows_ct, second_bit_first):
    replicas = lax.axis_size("dp")
    bits = replicas.bit_length() - 1
    me = lax.axis_index("dp")
    rows, width = rows_in.shape
    each = width // replicas

    def columns_of(bit):
        return jnp.concatenate(
            [
                lax.dynamic_slice_in_dim(rows_in, (2 * pair + bit) * each, each, axis=1)
                for pair in range(replicas // 2)
            ],
            axis=1,
        )

    mine = me % 2
    other = product(columns_of(1 - mine), rows_ct)
    held = product(columns_of(mine), rows_ct) + exchange(other, 0, replicas)
    left = list(range(bits - 1, 0, -1))
    cols = held.shape[1]
    held = held.reshape((2,) * len(left) + (each, cols))
    order = list(range(1, bits))
    if second_bit_first:
        order[:2] = order[:2][::-1]
    for bit in order:
        axis = left.index(bit)
        mine = (me // (1 << bit)) % 2
        sent = lax.dynamic_index_in_dim(held, 1 - mine, axis, keepdims=False)
        kept = lax.dynamic_index_in_dim(held, mine, axis, keepdims=False)
        held = kept + exchange(sent, bit, replicas)
        left.remove(bit)
    return held.reshape(each, cols)


def squared_total(values):
    return lax.psum(jnp.sum(values * values), ("dp", "mp"))


def shards(inputs, gate_cotangent, ff_blocks, layer_active, param, moment, second_moment):
    subnets, tokens, width = inputs.shape
    local_cols = gate_cotangent.shape[2]
    first_col = lax.axis_index("mp") * local_cols
    column = first_col + lax.broadcasted_iota(jnp.int32, (subnets, local_cols), 1)
    keep = (column < BLOCK * ff_blocks[:, None]) & (layer_active[:, None] == 1)
    masked = jnp.where(keep[:, None, :], gate_cotangent, jnp.zeros((), jnp.bfloat16))
    rows_in = inputs.reshape(subnets * tokens, width)
    rows_ct = masked.reshape(subnets * tokens, local_cols)
    tile = jnp.concatenate(
        [
            halving_sum(rows_in, part, second_bit_first=(place == CHUNKS - 1))
            for place, part in enumerate(jnp.split(rows_ct, CHUNKS, axis=1))
        ],
        axis=1,
    )
    owners = lax.axis_size("mp")
    pieces = lax.all_to_all(
        tile.reshape(owners, tile.shape[0] // owners, local_cols), "mp", split_axis=0, concat_axis=0
    )
    gradient = jnp.concatenate([pieces[i] for i in range(owners)], axis=1)
    total_sq = squared_total(gradient)
    total = jnp.sqrt(total_sq)
    factor = jnp.minimum(1.0, math.sqrt(1.0 * D * FF) / (total + 1e-06))
    clipped = gradient * factor
    new_moment = 0.9 * moment + 0.1 * clipped
    new_second = 0.95 * second_moment + 0.05 * clipped * clipped
    first_hat = new_moment / (1.0 - 0.9**STEP)
    second_hat = new_second / (1.0 - 0.95**STEP)
    new_param = param - 0.02 * (first_hat / (jnp.sqrt(second_hat) + 1e-08) + 0.1 * param)
    return (new_param, new_moment, new_second)


def solution(mesh):
    in_specs = (
        P(None, "dp", None),
        P(None, "dp", "mp"),
        P(),
        P(),
        P(("dp", "mp"), None),
        P(("dp", "mp"), None),
        P(("dp", "mp"), None),
    )
    out_specs = (P(("dp", "mp"), None), P(("dp", "mp"), None), P(("dp", "mp"), None))
    return jax.shard_map(shards, mesh=mesh, in_specs=in_specs, out_specs=out_specs, check_vma=False)
```
